32 devices in a mesh: dp: 2 (over y), ep: 16 (over z, x, core).
Axes of the slice: x: 2, y: 2, z: 4, core: 2. Of those that a mesh axis runs over, the one named last changes fastest.
Arguments:
- tokens: bfloat16 [3072, 2048], P(('dp', 'ep')), parts along dimension 0, may hold values from -6 to 6
- routes: int32 [3072, 8], P(('dp', 'ep')), parts along dimension 0, may hold values from 0 to 15, all different within a row; in each aligned block of 96 rows (0 to 95, 96 to 191, ...) at most 72 rows name the same one
- combine_weights: bfloat16 [3072, 8], P(('dp', 'ep')), parts along dimension 0, may hold values from 0.049804688 to 1
- w_gate: bfloat16 [16, 2048, 768], P('ep'), may hold values from -0.125 to 0.125
- w_up: bfloat16 [16, 2048, 768], P('ep'), may hold values from -0.125 to 0.125
- w_down: bfloat16 [16, 768, 2048], P('ep'), may hold values from -0.21875 to 0.21875
Outputs:
- mixed: bfloat16 [3072, 2048], P(('dp', 'ep')), parts along dimension 0
The draws below stay inside these ranges and needn't reach their ends.
There are 2 independent parts, one for each index of `dp`. The reference program is written for one: setup_inputs(seed, part) draws one part's arguments, and reference() takes and returns one part's arrays. A program takes and returns all parts, laid end to end along the dimension named above; an argument that names none is the same for every part. Nothing has to cross between parts.
Inputs may be any that keep to these rules, and one draw needn't show every extreme that they name: `routes`: each row names 8 different experts. Among the 96 rows of one device no expert is named by more than 72 rows, a bound that some blocks reach.
All inputs are finite; a program needn't handle non-finite values.
Results may differ from the reference program's by a relative error of at most 0.012.
Values may be sent and summed in bfloat16 or wider, within the bound.
A program may use at most 128 MiB of HBM per device.

```python
import math
import jax
import jax.numpy as jnp
import numpy as np
from jax import lax

D = 2048
FF = 768
TOP = 8
TOK_DEV = 96
EXPERTS = 16
CAP = 72
TOKENS = 1536
N_EP = 16


def shard_levels(key, extent, cuts, smallest, high):
    gain = 1.0
    for dim, shards_of in cuts:
        steps = jax.random.uniform(jax.random.fold_in(jax.random.fold_in(key, 6), dim), (shards_of,), jnp.float32, smallest / len(cuts), high / len(cuts))
        gain = gain * jnp.repeat(jnp.exp(steps), extent[dim] // shards_of).reshape((-1,) + (1,) * (len(extent) - 1 - dim))
    return gain


def routed_block(rng, own, number, rows, count, top, bound, skew):
    ranking = jax.random.permutation(rng, count)
    crowded, ordinary = load_shares(count, rows * top, bound, skew, True), load_shares(count, rows * top, bound, skew, False)
    places = jnp.arange(count)

    def named(tallies, turn):
        used = int((tallies > 0).sum())
        fixed = max(1, used // 4)
        moved = fixed + (places - fixed + turn * (used - fixed)) % max(1, count - fixed)
        return jnp.zeros((count,), jnp.int32).at[ranking[jnp.where(places < fixed, places, moved)]].set(jnp.asarray(tallies, jnp.int32))

    tallies = jnp.where(number % 4 == 0, named(crowded, number // 4), named(ordinary, number - number // 4 - 1))
    mixed = jax.random.permutation(jax.random.fold_in(own, 3), count)
    source_of, sink = mixed[0:count // 2 * 2:2], mixed[1:count // 2 * 2:2]
    slack = jnp.minimum(tallies[source_of] - 1, bound - tallies[sink]) // 2
    slack = jnp.where((source_of == ranking[0]) | (sink == ranking[0]) | (tallies[sink] == 0), 0, jnp.maximum(slack, 0))
    moved = jax.random.randint(jax.random.fold_in(own, 4), (count // 2,), 0, 1 << 20) % (slack + 1)
    tallies = tallies.at[source_of].add(-moved).at[sink].add(moved)
    members = jnp.searchsorted(jnp.cumsum(tallies), jnp.arange(rows * top), side="right").astype(jnp.int32)
    listing = members.reshape(top, rows).T
    listing = listing[jax.random.permutation(jax.random.fold_in(own, 1), rows)]
    turn = jax.random.randint(jax.random.fold_in(own, 2), (rows, 1), 0, top)
    return jnp.take_along_axis(listing, (jnp.arange(top)[None, :] + turn) % top, axis=1)


def load_shares(number_of, total, reach, skew, full):
    loads = [(1 << 20) // math.isqrt(grade ** skew) + 1 for grade in range(1, number_of + 1)]
    largest = reach if full else min(reach, max(-(-total // number_of), total * loads[0] // sum(loads)))
    least = 1 if total - largest >= number_of - 1 else 0
    given, spare = [largest] + [least] * (number_of - 1), total - largest - least * (number_of - 1)
    while spare > 0:
        candidates = [i for i in range(1, number_of) if given[i] < largest] or [i for i in range(1, number_of) if given[i] < reach]
        mass, budget = sum([loads[i] for i in candidates]), spare
        for i in candidates:
            more = min(reach - given[i], max(1, budget * loads[i] // mass), spare)
            given[i] = given[i] + more
            spare = spare - more
    return np.array(given)


def scatter_about(stream_key, extent, spread, limit, pieces=(), held_as=jnp.bfloat16):
    factor_of = shard_levels(stream_key, extent, pieces, -0.22, 0.18) if pieces else 1.0
    values = jax.random.normal(stream_key, extent, jnp.float32) * spread * factor_of
    return jnp.minimum(jnp.maximum(values, -limit), limit).astype(held_as)


def setup_inputs(seed: int = 0, part: int = 0) -> dict:
    key_list = jax.random.split(jax.random.key(seed), 7)
    own_keys = jax.random.split(jax.random.fold_in(key_list[6], part), 7)
    tokens = scatter_about(own_keys[0], (TOKENS, D), 1.0, 6.0, ((0, 16),))
    routes_keys = jax.random.split(jax.random.fold_in(own_keys[1], 1), TOKENS // TOK_DEV)
    routes_turns = jax.random.permutation(jax.random.fold_in(own_keys[1], 3), TOKENS // TOK_DEV)
    routes = jax.vmap(lambda own, number: routed_block(jax.random.fold_in(own_keys[1], 2), own, number, TOK_DEV, EXPERTS, TOP, CAP, 2))(routes_keys, routes_turns).reshape((TOKENS, TOP))
    combine_weights = jnp.clip(0.049804688 + 0.9501953 * jax.random.uniform(own_keys[2], (TOKENS, TOP), jnp.float32) ** shard_levels(own_keys[2], (TOKENS, TOP), ((0, 16),), -0.2, 0.2), 0.049804688, 1.0).astype(jnp.bfloat16)
    w_gate = scatter_about(key_list[3], (EXPERTS, D, FF), D ** -0.5, 0.125, ((0, 16),))
    w_up = scatter_about(key_list[4], (EXPERTS, D, FF), D ** -0.5, 0.125, ((0, 16),))
    w_down = scatter_about(key_list[5], (EXPERTS, FF, D), FF ** -0.5, 0.21875, ((0, 16),))
    return {"tokens": tokens, "routes": routes, "combine_weights": combine_weights, "w_gate": w_gate, "w_up": w_up, "w_down": w_down}


def expert_ffn(rows, row_weight, gate_matrix, upward_matrix, down_matrix):
    gate = jnp.dot(rows, gate_matrix, preferred_element_type=jnp.float32)
    upward = jnp.dot(rows, upward_matrix, preferred_element_type=jnp.float32)
    hidden = (jax.nn.silu(gate) * upward).astype(jnp.bfloat16)
    result = jnp.dot(hidden, down_matrix, preferred_element_type=jnp.float32)
    return (result * row_weight.astype(jnp.float32)[:, None]).astype(jnp.bfloat16)


def reference(tokens, routes, combine_weights, w_gate, w_up, w_down):
    pairs = TOKENS * TOP
    flat_routes = routes.reshape(-1)
    flat_weights = combine_weights.reshape(-1)
    room = N_EP * CAP

    def one_expert(total, expert):
        pair_index = jnp.nonzero(flat_routes == expert, size=room, fill_value=pairs)[0].astype(jnp.int32)
        token_index = (pair_index // TOP).astype(jnp.int32)
        rows = jnp.take(tokens, token_index, axis=0, mode="fill", fill_value=0)
        row_weight = jnp.take(flat_weights, pair_index, mode="fill", fill_value=0)
        result = expert_ffn(rows, row_weight, w_gate[expert], w_up[expert], w_down[expert])
        total = total.at[token_index].add(result.astype(jnp.float32), mode="drop")
        return total, None

    start = jnp.zeros((TOKENS, D), jnp.float32)
    total, unused = lax.scan(one_expert, start, jnp.arange(EXPERTS, dtype=jnp.int32))
    return total.astype(jnp.bfloat16)
```

```python
import functools

import jax
import jax.numpy as jnp
from jax import lax
from jax.experimental import pallas as pl
from jax.experimental.pallas import tpu as pltpu
from jax.sharding import PartitionSpec as P

MESH = pl.DeviceIdType.MESH


def fused_kernel(X, C, x_ref, wg_hbm, wu_hbm, wd_hbm, out_ref,
                 xall, yall, ysib, acc, arr, wg, wu, wd, hid,
                 w_sem, own_sem, xs_sem, xr_sem, ps_sem, pr_sem,
                 ys_sem, yr_sem, as_sem, ar_sem):
    Z = C // X
    N = C
    idx = lax.axis_index("ep")
    lane = idx % 2
    chip = idx // 2
    cx = chip % X
    cz = chip // X
    place = cx * Z + cz + (cx % 2) * (Z - 1 - 2 * cz)

    def device_at(r):
        x = r // Z
        t = r % Z
        z = t + (x % 2) * (Z - 1 - 2 * t)
        return (z * X + x) * 2 + lane

    right = device_at((place + 1) % C)
    left = device_at((place + C - 1) % C)
    other = idx + 1 - 2 * lane

    for src, dst, k in ((wg_hbm, wg, 0), (wu_hbm, wu, 1), (wd_hbm, wd, 2)):
        pltpu.make_async_copy(src.at[0], dst, w_sem.at[k]).start()
    own = pltpu.make_async_copy(x_ref, xall.at[0, lane], own_sem)
    own.start()

    barrier = pltpu.get_barrier_semaphore()
    for peer in (left, right, other):
        pl.semaphore_signal(barrier, inc=1, device_id={"ep": peer}, device_id_type=MESH)
    pl.semaphore_wait(barrier, 3)

    ahead = (right, left)
    behind = (left, right)

    def remote(src, dst, s, r, peer):
        return pltpu.make_async_remote_copy(
            src_ref=src, dst_ref=dst, send_sem=s, recv_sem=r,
            device_id={"ep": peer}, device_id_type=MESH)

    def token_copy(i, d):
        return remote(x_ref.at[min(i, 2) - 1], xall.at[i, lane, d], xs_sem.at[i, d], xr_sem.at[i, d], ahead[d])

    def pair_copy(i):
        src = x_ref if i == 0 else xall.at[i, lane]
        return remote(src, xall.at[i, lane], ps_sem.at[i], pr_sem.at[i], other)

    def partial_copy(i):
        return remote(yall.at[i, 1 - lane], ysib.at[i], ys_sem.at[i], yr_sem.at[i], other)

    def sum_copy(i, d):
        return remote(acc.at[i, d], arr.at[i, d], as_sem.at[i, d], ar_sem.at[i, d], behind[d])

    def continues(i, d):
        if i + 2 < N - 1:
            return True
        if i + 2 == N - 1:
            return d == 0
        if i + 2 == N:
            return d == 1
        return False

    def next_unit(i, d):
        return i + 2 if i + 2 <= N - 1 else N - 1

    def forward(i, d):
        k = next_unit(i, d)
        return remote(xall.at[i, lane, d], xall.at[k, lane, d],
                      xs_sem.at[k, d], xr_sem.at[k, d], ahead[d])

    width = wg.shape[0]
    hidden = wg.shape[1]
    half = x_ref.shape[1]
    rows = 4 * half
    ft = 256 if hidden % 256 == 0 else 128
    nt = 512 if width % 512 == 0 else 128

    def ffn(i):
        xw = xall[i, :, :, :, width:].reshape(rows, xall.shape[-1] - width).astype(jnp.float32)
        pick = lax.broadcasted_iota(jnp.int32, xw.shape, 1) == idx
        scale = jnp.sum(jnp.where(pick, xw, 0.0), axis=1, keepdims=True)

        @pl.loop(0, hidden // ft)
        def _(f):
            cols = pl.ds(pl.multiple_of(f * ft, ft), ft)
            xv = xall[i, :, :, :, :width].reshape(rows, width)
            g = jnp.dot(xv, wg[:, cols], preferred_element_type=jnp.float32)
            u = jnp.dot(xv, wu[:, cols], preferred_element_type=jnp.float32)
            hid[:, cols] = (g / (1.0 + jnp.exp(-g)) * u).astype(jnp.bfloat16)

        @pl.loop(0, width // nt)
        def _(n):
            cols = pl.ds(pl.multiple_of(n * nt, nt), nt)
            y = jnp.dot(hid[...], wd[:, cols], preferred_element_type=jnp.float32) * scale
            yall[i, :, :, :, cols] = y.astype(jnp.bfloat16).reshape(2, 2, half, nt)

    def reduce_send(i, d):
        total = yall[i, lane, d].astype(jnp.float32) + ysib[i, d].astype(jnp.float32)
        if continues(i, d):
            k = next_unit(i, d)
            sum_copy(k, d).wait_recv()
            total = total + arr[k, d].astype(jnp.float32)
        acc[i, d] = total.astype(jnp.bfloat16)
        sum_copy(i, d).start()

    for i in (1, 2):
        for d in (0, 1):
            token_copy(i, d).start()
    pair_copy(0).start()

    for i in range(N):
        if i > 0:
            for d in (0, 1):
                token_copy(i, d).wait_recv()
                if continues(i, d):
                    forward(i, d).start()
            pair_copy(i).start()
        else:
            own.wait()
            for src, dst, k in ((wg_hbm, wg, 0), (wu_hbm, wu, 1), (wd_hbm, wd, 2)):
                pltpu.make_async_copy(src.at[0], dst, w_sem.at[k]).wait()
        remote(xall.at[i, lane], xall.at[i, 1 - lane], ps_sem.at[i], pr_sem.at[i], other).wait_recv()
        if i == N - 1:
            partial_copy(N - 2).wait_recv()
            reduce_send(N - 2, 0)
        ffn(i)
        partial_copy(i).start()
        if i == N - 2:
            partial_copy(N - 3).wait_recv()
            reduce_send(N - 3, 1)

    for i in range(N - 3):
        partial_copy(i).wait_recv()
    partial_copy(N - 1).wait_recv()
    reduce_send(N - 1, 0)
    reduce_send(N - 1, 1)
    order = ([], [])
    for d in (0, 1):
        a, b = (N - 4, N - 3) if d == 0 else (N - 5, N - 2)
        while a >= 1 or b >= 1:
            if a >= 1:
                order[d].append(a)
            if b >= 1:
                order[d].append(b)
            a, b = a - 2, b - 2
    for s in range(max(len(order[0]), len(order[1]))):
        for d in (0, 1):
            if s < len(order[d]):
                reduce_send(order[d][s], d)

    for h in (0, 1):
        total = yall[0, lane, h].astype(jnp.float32) + ysib[0, h].astype(jnp.float32)
        for d in (0, 1):
            sum_copy(h + 1, d).wait_recv()
            total = total + arr[h + 1, d].astype(jnp.float32)
        out_ref[h] = total.astype(out_ref.dtype)

    for i in range(N):
        pair_copy(i).wait_send()
        partial_copy(i).wait_send()
        if i > 0:
            for d in (0, 1):
                token_copy(i, d).wait_send()
                sum_copy(i, d).wait_send()


def fused_local(X, tokens, routes, combine_weights, w_gate, w_up, w_down):
    peers = lax.axis_size("ep")
    local_tokens, width = tokens.shape
    hidden = w_gate.shape[2]
    C = peers // 2
    half = local_tokens // 2
    pad = -(-peers // 128) * 128
    names = jnp.arange(pad, dtype=jnp.int32)
    dense = jnp.sum(
        jnp.where(routes[:, :, None] == names[None, None, :],
                  combine_weights[:, :, None].astype(jnp.float32), 0.0), axis=1)
    x = jnp.concatenate([tokens, dense.astype(jnp.bfloat16)], axis=1)
    x = x.reshape(2, half, width + pad)
    bf = jnp.bfloat16
    dma = pltpu.SemaphoreType.DMA
    out = pl.pallas_call(
        functools.partial(fused_kernel, X, C),
        out_shape=jax.ShapeDtypeStruct((2, half, width), bf),
        in_specs=[pl.BlockSpec(memory_space=pltpu.VMEM)] + [pl.BlockSpec(memory_space=pl.ANY)] * 3,
        out_specs=pl.BlockSpec(memory_space=pltpu.VMEM),
        scratch_shapes=[
            pltpu.VMEM((C, 2, 2, half, width + pad), bf),
            pltpu.VMEM((C, 2, 2, half, width), bf),
            pltpu.VMEM((C, 2, half, width), bf),
            pltpu.VMEM((C, 2, half, width), bf),
            pltpu.VMEM((C, 2, half, width), bf),
            pltpu.VMEM((width, hidden), bf),
            pltpu.VMEM((width, hidden), bf),
            pltpu.VMEM((hidden, width), bf),
            pltpu.VMEM((4 * half, hidden), bf),
            dma((3,)), dma,
            dma((C, 2)), dma((C, 2)), dma((C,)), dma((C,)),
            dma((C,)), dma((C,)), dma((C, 2)), dma((C, 2)),
        ],
        compiler_params=pltpu.CompilerParams(collective_id=0, has_side_effects=True),
    )(x, w_gate, w_up, w_down)
    return out.reshape(local_tokens, width)


def expert_ffn(rows, row_weight, gate_matrix, upward_matrix, down_matrix):
    gate = jnp.dot(rows, gate_matrix, preferred_element_type=jnp.float32)
    upward = jnp.dot(rows, upward_matrix, preferred_element_type=jnp.float32)
    hidden = (jax.nn.silu(gate) * upward).astype(jnp.bfloat16)
    result = jnp.dot(hidden, down_matrix, preferred_element_type=jnp.float32)
    return (result * row_weight.astype(jnp.float32)[:, None]).astype(jnp.bfloat16)


def run_expert(arrived, arrived_weight, gate_matrix, upward_matrix, down_matrix):
    sources, slots, width = arrived.shape
    rows = arrived.reshape(sources * slots, width)
    row_weight = arrived_weight.reshape(sources * slots)
    output = expert_ffn(rows, row_weight, gate_matrix, upward_matrix, down_matrix)
    return output.reshape(sources, slots, width)


def local(tokens, routes, combine_weights, w_gate, w_up, w_down):
    peers = lax.axis_size("ep")
    local_tokens, width = tokens.shape
    top_count = routes.shape[1]
    room = min(local_tokens, 3 * local_tokens * top_count // (2 * peers))
    pair_count = local_tokens * top_count
    flat_routes = routes.reshape(-1)
    one_hot = (flat_routes[:, None] == jnp.arange(peers, dtype=jnp.int32)[None, :]).astype(
        jnp.int32
    )
    earlier = jnp.cumsum(one_hot, axis=0) - one_hot
    position = jnp.sum(earlier * one_hot, axis=1)
    slot_index = flat_routes * room + position
    owner = jnp.full((peers * room,), pair_count, jnp.int32)
    owner = owner.at[slot_index].set(jnp.arange(pair_count, dtype=jnp.int32))
    send_rows = jnp.take(tokens, owner // top_count, axis=0, mode="fill", fill_value=0)
    send_rows = send_rows.reshape(peers, room, width)
    send_weight = jnp.take(combine_weights.reshape(-1), owner, mode="fill", fill_value=0)
    send_weight = send_weight.reshape(peers, room)
    gate_matrix = w_gate[0]
    upward_matrix = w_up[0]
    down_matrix = w_down[0]
    arrived, arrived_weight = (
        lax.all_to_all(send_rows, "ep", split_axis=0, concat_axis=0, tiled=True),
        lax.all_to_all(send_weight, "ep", split_axis=0, concat_axis=0, tiled=True),
    )
    output = run_expert(arrived, arrived_weight, gate_matrix, upward_matrix, down_matrix)
    back = lax.all_to_all(output, "ep", split_axis=0, concat_axis=0, tiled=True)
    back_rows = back.reshape(peers * room, width)
    per_pair = jnp.take(back_rows, slot_index, axis=0)
    summed = jnp.sum(per_pair.reshape(local_tokens, top_count, width).astype(jnp.float32), axis=1)
    return summed.astype(jnp.bfloat16)


def solution(mesh):
    in_specs = (
        P(("dp", "ep"), None),
        P(("dp", "ep"), None),
        P(("dp", "ep"), None),
        P("ep", None, None),
        P("ep", None, None),
        P("ep", None, None),
    )
    out_specs = P(("dp", "ep"), None)
    peers, X = mesh.shape["ep"], mesh.shape["dp"]

    def layer(tokens, routes, *rest):
        count = tokens.shape[0]
        dense = peers <= 2 * routes.shape[1] and peers % (4 * X) == 0 and count % 32 == 0
        body = functools.partial(fused_local, X) if dense and peers >= 8 else local
        return body(tokens, routes, *rest)

    return jax.shard_map(layer, mesh=mesh, in_specs=in_specs, out_specs=out_specs, check_vma=False)
```

```python
import functools

import jax
import jax.numpy as jnp
from jax import lax
from jax.experimental import pallas as pl
from jax.experimental.pallas import tpu as pltpu
from jax.sharding import PartitionSpec as P

MESH = pl.DeviceIdType.MESH


def fused_kernel(X, C, x_hbm, c_hbm, wg_hbm, wu_hbm, wd_hbm, out_ref,
                 xall, yall, ysib, acc, arr, wg, wu, wd, hid,
                 w_sem, own_sem, xs_sem, xr_sem, ps_sem, pr_sem,
                 ys_sem, yr_sem, as_sem, ar_sem):
    Z = C // X
    N = C
    idx = lax.axis_index("ep")
    lane = idx % 2
    chip = idx // 2
    cx = chip % X
    cz = chip // X
    place = cx * Z + cz + (cx % 2) * (Z - 1 - 2 * cz)

    def device_at(r):
        x = r // Z
        t = r % Z
        z = t + (x % 2) * (Z - 1 - 2 * t)
        return (z * X + x) * 2 + lane

    right = device_at((place + 1) % C)
    left = device_at((place + C - 1) % C)
    other = idx + 1 - 2 * lane

    width = wg.shape[0]
    half = xall.shape[3]
    pad = xall.shape[4] - width
    own = (
        pltpu.make_async_copy(x_hbm, xall.at[0, lane, :, :, pl.ds(0, width)], own_sem.at[0]),
        pltpu.make_async_copy(c_hbm, xall.at[0, lane, :, :, pl.ds(width, pad)], own_sem.at[1]),
    )
    weights = [pltpu.make_async_copy(src.at[0], dst, w_sem.at[k])
               for src, dst, k in ((wg_hbm, wg, 0), (wu_hbm, wu, 1), (wd_hbm, wd, 2))]
    for copy in own:
        copy.start()
    for copy in weights:
        copy.start()

    barrier = pltpu.get_barrier_semaphore()
    for peer in (left, right, other):
        pl.semaphore_signal(barrier, inc=1, device_id={"ep": peer}, device_id_type=MESH)
    pl.semaphore_wait(barrier, 3)

    ahead = (right, left)
    behind = (left, right)

    def remote(src, dst, s, r, peer):
        return pltpu.make_async_remote_copy(
            src_ref=src, dst_ref=dst, send_sem=s, recv_sem=r,
            device_id={"ep": peer}, device_id_type=MESH)

    def token_copy(i, d):
        return remote(xall.at[0, lane, min(i, 2) - 1], xall.at[i, lane, d], xs_sem.at[i, d], xr_sem.at[i, d], ahead[d])

    def pair_copy(i):
        return remote(xall.at[i, lane], xall.at[i, lane], ps_sem.at[i], pr_sem.at[i], other)

    def partial_copy(i):
        return remote(yall.at[i, 1 - lane], ysib.at[i], ys_sem.at[i], yr_sem.at[i], other)

    def sum_copy(i, d):
        return remote(acc.at[i, d], arr.at[i, d], as_sem.at[i, d], ar_sem.at[i, d], behind[d])

    def continues(i, d):
        if i + 2 < N - 1:
            return True
        if i + 2 == N - 1:
            return d == 0
        if i + 2 == N:
            return d == 1
        return False

    def next_unit(i, d):
        return i + 2 if i + 2 <= N - 1 else N - 1

    def forward(i, d):
        k = next_unit(i, d)
        return remote(xall.at[i, lane, d], xall.at[k, lane, d],
                      xs_sem.at[k, d], xr_sem.at[k, d], ahead[d])

    rows = 4 * half

    def ffn(i):
        xw = xall[i, :, :, :, width:].reshape(rows, pad).astype(jnp.float32)
        pick = lax.broadcasted_iota(jnp.int32, xw.shape, 1) == idx
        scale = jnp.sum(jnp.where(pick, xw, 0.0), axis=1, keepdims=True)

        xv = xall[i, :, :, :, :width].reshape(rows, width)
        g = jnp.dot(xv, wg[...], preferred_element_type=jnp.float32)
        u = jnp.dot(xv, wu[...], preferred_element_type=jnp.float32)
        hid[...] = (g / (1.0 + jnp.exp(-g)) * u).astype(jnp.bfloat16)
        y = jnp.dot(hid[...], wd[...], preferred_element_type=jnp.float32) * scale
        yall[i] = y.astype(jnp.bfloat16).reshape(2, 2, half, width)

    def reduce_send(i, d):
        total = yall[i, lane, d].astype(jnp.float32) + ysib[i, d].astype(jnp.float32)
        if continues(i, d):
            k = next_unit(i, d)
            sum_copy(k, d).wait_recv()
            total = total + arr[k, d].astype(jnp.float32)
        acc[i, d] = total.astype(jnp.bfloat16)
        sum_copy(i, d).start()

    for copy in own:
        copy.wait()
    for i in (1, 2):
        for d in (0, 1):
            token_copy(i, d).start()
    pair_copy(0).start()

    for i in range(N):
        if i > 0:
            for d in (0, 1):
                token_copy(i, d).wait_recv()
                if continues(i, d):
                    forward(i, d).start()
            pair_copy(i).start()
        else:
            for copy in weights:
                copy.wait()
        remote(xall.at[i, lane], xall.at[i, 1 - lane], ps_sem.at[i], pr_sem.at[i], other).wait_recv()
        if i == N - 1:
            partial_copy(N - 2).wait_recv()
            reduce_send(N - 2, 0)
        ffn(i)
        partial_copy(i).start()
        if i == N - 2:
            partial_copy(N - 3).wait_recv()
            reduce_send(N - 3, 1)

    for i in range(N - 3):
        partial_copy(i).wait_recv()
    partial_copy(N - 1).wait_recv()
    reduce_send(N - 1, 0)
    reduce_send(N - 1, 1)
    order = ([], [])
    for d in (0, 1):
        a, b = (N - 4, N - 3) if d == 0 else (N - 5, N - 2)
        while a >= 1 or b >= 1:
            if a >= 1:
                order[d].append(a)
            if b >= 1:
                order[d].append(b)
            a, b = a - 2, b - 2
    for s in range(max(len(order[0]), len(order[1]))):
        for d in (0, 1):
            if s < len(order[d]):
                reduce_send(order[d][s], d)

    for h in (0, 1):
        total = yall[0, lane, h].astype(jnp.float32) + ysib[0, h].astype(jnp.float32)
        for d in (0, 1):
            sum_copy(h + 1, d).wait_recv()
            total = total + arr[h + 1, d].astype(jnp.float32)
        out_ref[h] = total.astype(out_ref.dtype)

    for i in range(N):
        pair_copy(i).wait_send()
        partial_copy(i).wait_send()
        if i > 0:
            for d in (0, 1):
                token_copy(i, d).wait_send()
                sum_copy(i, d).wait_send()


def fused_local(X, tokens, routes, combine_weights, w_gate, w_up, w_down):
    peers = lax.axis_size("ep")
    local_tokens, width = tokens.shape
    hidden = w_gate.shape[2]
    C = peers // 2
    half = local_tokens // 2
    pad = -(-peers // 128) * 128
    names = jnp.arange(pad, dtype=jnp.int32)
    dense = jnp.sum(
        jnp.where(routes[:, :, None] == names[None, None, :],
                  combine_weights[:, :, None].astype(jnp.float32), 0.0), axis=1)
    dense = dense.astype(jnp.bfloat16).reshape(2, half, pad)
    x = tokens.reshape(2, half, width)
    bf = jnp.bfloat16
    dma = pltpu.SemaphoreType.DMA
    out = pl.pallas_call(
        functools.partial(fused_kernel, X, C),
        out_shape=jax.ShapeDtypeStruct((2, half, width), bf),
        in_specs=[pl.BlockSpec(memory_space=pl.ANY)] * 5,
        out_specs=pl.BlockSpec(memory_space=pltpu.VMEM),
        scratch_shapes=[
            pltpu.VMEM((C, 2, 2, half, width + pad), bf),
            pltpu.VMEM((C, 2, 2, half, width), bf),
            pltpu.VMEM((C, 2, half, width), bf),
            pltpu.VMEM((C, 2, half, width), bf),
            pltpu.VMEM((C, 2, half, width), bf),
            pltpu.VMEM((width, hidden), bf),
            pltpu.VMEM((width, hidden), bf),
            pltpu.VMEM((hidden, width), bf),
            pltpu.VMEM((4 * half, hidden), bf),
            dma((3,)), dma((2,)),
            dma((C, 2)), dma((C, 2)), dma((C,)), dma((C,)),
            dma((C,)), dma((C,)), dma((C, 2)), dma((C, 2)),
        ],
        compiler_params=pltpu.CompilerParams(collective_id=0, has_side_effects=True),
    )(x, dense, w_gate, w_up, w_down)
    return out.reshape(local_tokens, width)


def expert_ffn(rows, row_weight, gate_matrix, upward_matrix, down_matrix):
    gate = jnp.dot(rows, gate_matrix, preferred_element_type=jnp.float32)
    upward = jnp.dot(rows, upward_matrix, preferred_element_type=jnp.float32)
    hidden = (jax.nn.silu(gate) * upward).astype(jnp.bfloat16)
    result = jnp.dot(hidden, down_matrix, preferred_element_type=jnp.float32)
    return (result * row_weight.astype(jnp.float32)[:, None]).astype(jnp.bfloat16)


def run_expert(arrived, arrived_weight, gate_matrix, upward_matrix, down_matrix):
    sources, slots, width = arrived.shape
    rows = arrived.reshape(sources * slots, width)
    row_weight = arrived_weight.reshape(sources * slots)
    output = expert_ffn(rows, row_weight, gate_matrix, upward_matrix, down_matrix)
    return output.reshape(sources, slots, width)


def local(tokens, routes, combine_weights, w_gate, w_up, w_down):
    peers = lax.axis_size("ep")
    local_tokens, width = tokens.shape
    top_count = routes.shape[1]
    room = min(local_tokens, 3 * local_tokens * top_count // (2 * peers))
    pair_count = local_tokens * top_count
    flat_routes = routes.reshape(-1)
    one_hot = (flat_routes[:, None] == jnp.arange(peers, dtype=jnp.int32)[None, :]).astype(
        jnp.int32
    )
    earlier = jnp.cumsum(one_hot, axis=0) - one_hot
    position = jnp.sum(earlier * one_hot, axis=1)
    slot_index = flat_routes * room + position
    owner = jnp.full((peers * room,), pair_count, jnp.int32)
    owner = owner.at[slot_index].set(jnp.arange(pair_count, dtype=jnp.int32))
    send_rows = jnp.take(tokens, owner // top_count, axis=0, mode="fill", fill_value=0)
    send_rows = send_rows.reshape(peers, room, width)
    send_weight = jnp.take(combine_weights.reshape(-1), owner, mode="fill", fill_value=0)
    send_weight = send_weight.reshape(peers, room)
    gate_matrix = w_gate[0]
    upward_matrix = w_up[0]
    down_matrix = w_down[0]
    arrived, arrived_weight = (
        lax.all_to_all(send_rows, "ep", split_axis=0, concat_axis=0, tiled=True),
        lax.all_to_all(send_weight, "ep", split_axis=0, concat_axis=0, tiled=True),
    )
    output = run_expert(arrived, arrived_weight, gate_matrix, upward_matrix, down_matrix)
    back = lax.all_to_all(output, "ep", split_axis=0, concat_axis=0, tiled=True)
    back_rows = back.reshape(peers * room, width)
    per_pair = jnp.take(back_rows, slot_index, axis=0)
    summed = jnp.sum(per_pair.reshape(local_tokens, top_count, width).astype(jnp.float32), axis=1)
    return summed.astype(jnp.bfloat16)


def solution(mesh):
    in_specs = (
        P(("dp", "ep"), None),
        P(("dp", "ep"), None),
        P(("dp", "ep"), None),
        P("ep", None, None),
        P("ep", None, None),
        P("ep", None, None),
    )
    out_specs = P(("dp", "ep"), None)
    peers, X = mesh.shape["ep"], mesh.shape["dp"]

    def layer(tokens, routes, *rest):
        count = tokens.shape[0]
        dense = peers <= 2 * routes.shape[1] and peers % (4 * X) == 0 and count % 32 == 0
        body = functools.partial(fused_local, X) if dense and peers >= 8 else local
        return body(tokens, routes, *rest)

    return jax.shard_map(layer, mesh=mesh, in_specs=in_specs, out_specs=out_specs, check_vma=False)
```
